32 devices in a mesh: lat: 8 (over z, y), lon: 4 (over x, core).
Axes of the slice: x: 2, y: 2, z: 4, core: 2. Of those that a mesh axis runs over, the one named last changes fastest.
Arguments:
- predicted_state: bfloat16 [222, 320, 512], P(None, 'lat', 'lon'), may hold values from -30 to 30
- observed_state: bfloat16 [222, 320, 512], P(None, 'lat', 'lon'), may hold values from -30 to 30
- longterm_average_state: bfloat16 [222, 320, 512], P(None, 'lat', 'lon'), may hold values from -30 to 30
Outputs:
- blurred_mismatch_map: bfloat16 [222, 320, 512], P(None, 'lat', 'lon')
- quadratic_mean_mistake: float32 [222], replicated
- pattern_agreement: float32 [222], replicated
The draws below stay inside these ranges and needn't reach their ends.
All inputs are finite; a program needn't handle non-finite values.
Results may differ from the reference program's by a relative error of at most 0.00155.
Values may be sent and summed in bfloat16 or wider, within the bound.
A program may use at most 128 MiB of HBM per device.

```python
import jax
import jax.numpy as jnp
from jax import lax

FIELDS = 222
NLAT = 320
NLON = 512


def joint_fields(key):
    base = jax.random.fold_in(key, 11)
    key_climate, key_anomaly, random_seed_mistake = jax.random.split(base, 3)
    mesh_dimensions = (FIELDS, NLAT, NLON)
    lat_frac = jnp.arange(NLAT, dtype=jnp.float32) / (NLAT - 1)
    lon_frac = jnp.arange(NLON, dtype=jnp.float32) / (NLON - 1)
    anomaly_strength = (1.0 + 2.0 * lat_frac)[:, None] * (1.0 + 2.0 * lon_frac)[None, :] / 3.0
    normal_reference_state = 2.0 * jax.random.normal(key_climate, mesh_dimensions, dtype=jnp.float32)
    anomaly = jax.random.normal(key_anomaly, mesh_dimensions, dtype=jnp.float32)
    prediction_mismatch = 0.7 * jax.random.normal(random_seed_mistake, mesh_dimensions, dtype=jnp.float32)
    observed_state = normal_reference_state + anomaly
    predicted_state = observed_state + prediction_mismatch * anomaly_strength
    return (jnp.clip(predicted_state, -30.0, 30.0), jnp.clip(observed_state, -30.0, 30.0), jnp.clip(normal_reference_state, -30.0, 30.0))


def draw_predicted_state(key, part):
    return joint_fields(key)[0].astype(jnp.bfloat16)


def draw_observed_state(key, part):
    return joint_fields(key)[1].astype(jnp.bfloat16)


def draw_longterm_average_state(key, part):
    return joint_fields(key)[2].astype(jnp.bfloat16)


def setup_inputs(seed: int = 0) -> dict:
    seeds = jax.random.split(jax.random.key(seed), 4)
    predicted_state = draw_predicted_state(jax.random.fold_in(seeds[3], 71), 0)
    observed_state = draw_observed_state(jax.random.fold_in(seeds[3], 71), 0)
    longterm_average_state = draw_longterm_average_state(jax.random.fold_in(seeds[3], 71), 0)
    return dict(predicted_state=predicted_state, observed_state=observed_state, longterm_average_state=longterm_average_state)


epsilon = 1e-06

def finish(running_accumulations, grid_cells):
    mean_fcst = running_accumulations[1] / grid_cells
    mean_true = running_accumulations[2] / grid_cells
    variance_fcst = running_accumulations[3] / grid_cells - mean_fcst * mean_fcst
    variance_true = running_accumulations[4] / grid_cells - mean_true * mean_true
    covariance = running_accumulations[5] / grid_cells - mean_fcst * mean_true
    quadratic_mean_mistake = jnp.sqrt(running_accumulations[0] / grid_cells)
    pattern_agreement = covariance / jnp.sqrt((variance_fcst + epsilon) * (variance_true + epsilon))
    return (quadratic_mean_mistake, pattern_agreement)

def reference(predicted_state, observed_state, longterm_average_state):
    parallel_overall_accumulated = predicted_state.shape[1]
    meridian_accumulated = predicted_state.shape[2]
    row_index = jnp.arange(parallel_overall_accumulated, dtype=jnp.int32)
    all_rows = jnp.arange(parallel_overall_accumulated, dtype=jnp.float32)
    cosine = jnp.cos(jnp.pi * (0.5 - all_rows / (parallel_overall_accumulated - 1)))
    cosine_factor_vector = (cosine / jnp.mean(cosine))[:, None]
    row_count = 3.0 - (row_index == 0).astype(jnp.float32) - (row_index == parallel_overall_accumulated - 1).astype(jnp.float32)
    divisor = (3.0 * row_count)[:, None]

    def smooth(member):
        padded = jnp.pad(member, ((1, 1), (0, 0)))
        vertical = padded[:-2] + padded[1:-1] + padded[2:]
        horizontal = jnp.roll(vertical, 1, 1) + vertical + jnp.roll(vertical, -1, 1)
        return horizontal / divisor

    def lone_variable_entry(members):
        normal_reference_state = members[2].astype(jnp.float32)
        averaged_prediction = smooth(members[0].astype(jnp.float32) - normal_reference_state)
        averaged_observation = smooth(members[1].astype(jnp.float32) - normal_reference_state)
        prediction_mismatch = averaged_prediction - averaged_observation
        running_accumulations = jnp.stack([jnp.sum(cosine_factor_vector * prediction_mismatch * prediction_mismatch), jnp.sum(cosine_factor_vector * averaged_prediction), jnp.sum(cosine_factor_vector * averaged_observation), jnp.sum(cosine_factor_vector * averaged_prediction * averaged_prediction), jnp.sum(cosine_factor_vector * averaged_observation * averaged_observation), jnp.sum(cosine_factor_vector * averaged_prediction * averaged_observation)])
        return (prediction_mismatch.astype(jnp.bfloat16), running_accumulations)
    blurred_mismatch_map, running_accumulations = lax.map(lone_variable_entry, (predicted_state, observed_state, longterm_average_state))
    quadratic_mean_mistake, pattern_agreement = finish(jnp.transpose(running_accumulations), float(parallel_overall_accumulated * meridian_accumulated))
    return (blurred_mismatch_map, quadratic_mean_mistake, pattern_agreement)
```

```python
import functools

import jax
import jax.numpy as jnp
import numpy as np
from jax import lax
from jax.experimental import pallas as pl
from jax.experimental.pallas import tpu as pltpu
from jax.sharding import PartitionSpec as P

MESH = pl.DeviceIdType.MESH
LANES = 128
PAIRS = LANES // 2
epsilon = 1e-06


def lane_index(shape):
    return lax.broadcasted_iota(jnp.int32, shape, len(shape) - 1)


def around(axis, step, size):
    return lax.rem(lax.axis_index(axis) + (step + size), size)


def exchange_kernel(nlat, nlon, p_ref, o_ref, c_ref, g_ref, h_ref, tiles, q, ct, cb, rows, qr, cr, rr, send, recv):
    fields, height, width = p_ref.shape
    chunks = pl.cdiv(fields, PAIRS)
    blocks = width // LANES
    down, up = around("lat", 1, nlat), around("lat", -1, nlat)
    right, left = around("lon", 1, nlon), around("lon", -1, nlon)
    y, x = lax.axis_index("lat"), lax.axis_index("lon")
    routes = [
        (q, qr.at[0], (y, right)),
        (q, qr.at[1], (y, left)),
        (rows.at[1], rr.at[0], (down, x)),
        (rows.at[0], rr.at[1], (up, x)),
        (ct, cr.at[0], (down, right)),
        (ct, cr.at[1], (down, left)),
        (cb, cr.at[2], (up, right)),
        (cb, cr.at[3], (up, left)),
    ]
    barrier = pltpu.get_barrier_semaphore()
    for _, _, target in routes:
        pl.semaphore_signal(barrier, inc=1, device_id=target, device_id_type=MESH)

    lane = lane_index((height, LANES))
    for chunk in range(chunks):
        count = min(PAIRS, fields - chunk * PAIRS)

        def pack(j, totals):
            f = chunk * PAIRS + j
            keep = (lane >> 1) == j
            out = []
            for a, ref in enumerate((p_ref, o_ref, c_ref)):
                cells = ref[f].astype(jnp.float32)
                at = pl.multiple_of(f * 8, 8)
                for b in range(blocks):
                    cut = slice(b * LANES, (b + 1) * LANES)
                    tiles[0, a, b, pl.ds(at, 8), :] = cells[:8, cut]
                    tiles[1, a, b, pl.ds(at, 8), :] = cells[height - 8 :, cut]
                edge = cells
                if blocks > 1:
                    edge = jnp.where(lane == 0, cells[:, :LANES], cells[:, width - LANES :])
                out.append(jnp.where(keep, pltpu.roll(edge, 2 * j + 1, axis=1), totals[a]))
            return tuple(out)

        zero = jnp.zeros((height, LANES), jnp.float32)
        packed = lax.fori_loop(0, count, pack, (zero, zero, zero), unroll=2 if count % 2 == 0 else 1)
        for a in range(3):
            q[a, chunk] = packed[a].astype(jnp.bfloat16)
            ct[a, chunk] = packed[a][height - 8 :].astype(jnp.bfloat16)
            cb[a, chunk] = packed[a][:8].astype(jnp.bfloat16)
    for side, row in ((0, 0), (1, 7)):
        for a in range(3):
            for b in range(blocks):
                line = tiles[side, a, b, pl.ds(row, fields, stride=8), :]
                rows[side, a, pl.ds(0, fields), b * LANES : (b + 1) * LANES] = line.astype(jnp.bfloat16)

    pl.semaphore_wait(barrier, len(routes))
    copies = [
        pltpu.make_async_remote_copy(
            src_ref=src, dst_ref=dst, send_sem=send.at[i], recv_sem=recv.at[i], device_id=target, device_id_type=MESH
        )
        for i, (src, dst, target) in enumerate(routes)
    ]
    for copy in copies:
        copy.start()
    for copy in copies:
        copy.wait()

    inside = ((y > 0).astype(jnp.float32), (y < nlat - 1).astype(jnp.float32))

    def merged(west, east):
        shape = west[0].shape
        even = (lane_index(shape) & 1) == 0
        picked = [jnp.where(even, l.astype(jnp.float32), r.astype(jnp.float32)) for l, r in zip(west, east)]
        out = []
        for a in range(2):
            d = picked[a] - picked[2]
            out.append(jnp.where(even, pltpu.roll(d, LANES - 1, axis=1), pltpu.roll(d, 1, axis=1)))
        return out

    for chunk in range(chunks):
        mid = merged([qr[0, a, chunk] for a in range(3)], [qr[1, a, chunk] for a in range(3)])
        top = merged([cr[0, a, chunk] for a in range(3)], [cr[1, a, chunk] for a in range(3)])
        bottom = merged([cr[2, a, chunk] for a in range(3)], [cr[3, a, chunk] for a in range(3)])
        for a in range(2):
            g_ref[a, chunk, pl.ds(0, 8), :] = top[a] * inside[0]
            g_ref[a, chunk, pl.ds(8, height), :] = mid[a]
            g_ref[a, chunk, pl.ds(8 + height, 8), :] = bottom[a] * inside[1]
    wide = lane_index((fields, width))
    for side in range(2):
        line = [rr[side, a, pl.ds(0, fields), :].astype(jnp.float32) for a in range(3)]
        for a in range(2):
            d = line[a] - line[2]
            before = jnp.where(wide == 0, 0.0, pltpu.roll(d, 1, axis=1))
            after = jnp.where(wide == width - 1, 0.0, pltpu.roll(d, width - 1, axis=1))
            h_ref[a, side, pl.ds(0, fields), :] = (d + before + after) * inside[side]


def stencil_kernel(nlat, group, p_ref, o_ref, c_ref, g_ref, h_ref, m_ref, s_ref, hs, acc, wr):
    step = pl.program_id(0)
    block, height, width = p_ref.shape
    fields = block * pl.num_programs(0)
    blocks = width // LANES
    total_rows = nlat * height

    @pl.when(step == 0)
    def _():
        row = lax.axis_index("lat") * height + lax.broadcasted_iota(jnp.int32, (height, width), 0)
        spots = np.arange(total_rows, dtype=np.float64) / (total_rows - 1)
        mean = float(np.mean(np.cos(np.pi * (0.5 - spots))))
        place = row.astype(jnp.float32) / (total_rows - 1)
        wr[0] = jnp.cos(jnp.pi * (0.5 - place)) / mean
        count = 3.0 - (row == 0).astype(jnp.float32) - (row == total_rows - 1).astype(jnp.float32)
        wr[1] = 1.0 / (3.0 * count)

    lane = lane_index((height, width))
    first, last = lane == 0, lane == width - 1
    line = lane_index((1, width))
    ends = (line == 0) | (line == width - 1)

    def body(g, carry):
        weight, inverse = wr[0], wr[1]
        for u in range(group):
            local = g * group + u
            f = step * block + local
            chunk, j = f // PAIRS, lax.rem(f, PAIRS)
            normal = c_ref[local].astype(jnp.float32)
            smooth = []
            for a, ref in enumerate((p_ref, o_ref)):
                d = ref[local].astype(jnp.float32) - normal
                edge = pltpu.roll(g_ref[a, chunk], LANES - 1 - 2 * j, axis=1)
                if blocks > 1:
                    edge = jnp.concatenate([edge] * blocks, axis=1)
                mid = edge[8 : 8 + height]
                hs[u, a, 8 : 8 + height, :] = (
                    d
                    + jnp.where(first, mid, pltpu.roll(d, 1, axis=1))
                    + jnp.where(last, mid, pltpu.roll(d, width - 1, axis=1))
                )
                hs[u, a, 7:8, :] = h_ref[a, 0, pl.ds(f, 1), :] + jnp.where(ends, edge[7:8], 0.0)
                hs[u, a, 8 + height : 9 + height, :] = h_ref[a, 1, pl.ds(f, 1), :] + jnp.where(
                    ends, edge[8 + height : 9 + height], 0.0
                )
                box = hs[u, a, 7 : 7 + height, :] + hs[u, a, 8 : 8 + height, :] + hs[u, a, 9 : 9 + height, :]
                smooth.append(box * inverse)
            fcst, true = smooth
            gap = fcst - true
            m_ref[local] = gap.astype(jnp.bfloat16)
            wf, wt = weight * fcst, weight * true
            at = pl.multiple_of(f * 8, 8)
            for k, term in enumerate((weight * gap * gap, wf, wt, wf * fcst, wt * true, wf * true)):
                part = jnp.sum(term.reshape(height // 8, 8, width), axis=0)
                if blocks > 1:
                    part = sum(part[:, b * LANES : (b + 1) * LANES] for b in range(blocks))
                acc[k, pl.ds(at, 8), :] = part
        return carry

    lax.fori_loop(0, block // group, body, 0)

    @pl.when(step == pl.num_programs(0) - 1)
    def _():
        ones = jnp.ones((8, LANES), jnp.float32)
        count = acc.shape[1] // 8
        s_ref[...] = jnp.zeros_like(s_ref)
        for k in range(6):
            part = acc[k, pl.ds(0, count, stride=8), :]
            for s in range(1, 8):
                part = part + acc[k, pl.ds(s, count, stride=8), :]
            r = lax.dot_general(
                ones, part, (((1,), (1,)), ((), ())), precision=lax.Precision.HIGHEST, preferred_element_type=jnp.float32
            )
            s_ref[k : k + 1, pl.ds(0, count)] = r[:1]


def total_kernel(nlat, nlon, cells, s_ref, e_ref, a_ref, b1, b2, t1, send1, recv1, send2, recv2):
    y, x = lax.axis_index("lat"), lax.axis_index("lon")
    barrier = pltpu.get_barrier_semaphore()
    for d in range(1, nlon):
        pl.semaphore_signal(barrier, inc=1, device_id=(y, around("lon", d, nlon)), device_id_type=MESH)
    for d in range(1, nlat):
        pl.semaphore_signal(barrier, inc=1, device_id=(around("lat", d, nlat), x), device_id_type=MESH)
    pl.semaphore_wait(barrier, nlon - 1 + nlat - 1)

    def stage(src, buf, send, recv, axis, size, me):
        def copy(d, slot):
            peer = around(axis, d, size)
            target = (y, peer) if axis == "lon" else (peer, x)
            return pltpu.make_async_remote_copy(
                src_ref=src,
                dst_ref=buf.at[slot],
                send_sem=send.at[d],
                recv_sem=recv.at[slot],
                device_id=target,
                device_id_type=MESH,
            )

        for d in range(1, size):
            copy(d, me).start()
        buf[me] = src[...]
        for d in range(1, size):
            copy(d, around(axis, -d, size)).wait_recv()
        total = buf[0]
        for i in range(1, size):
            total = total + buf[i]
        for d in range(1, size):
            copy(d, me).wait_send()
        return total

    t1[...] = stage(s_ref, b1, send1, recv1, "lon", nlon, x)
    totals = stage(t1, b2, send2, recv2, "lat", nlat, y)
    n = e_ref.shape[1]
    part = [totals[k : k + 1, :n] / cells for k in range(6)]
    variance_fcst = part[3] - part[1] * part[1]
    variance_true = part[4] - part[2] * part[2]
    covariance = part[5] - part[1] * part[2]
    e_ref[...] = jnp.sqrt(part[0])
    a_ref[...] = covariance / jnp.sqrt((variance_fcst + epsilon) * (variance_true + epsilon))


def largest_divisor(n, limit):
    return max(d for d in range(1, limit + 1) if n % d == 0)


def local(nlat, nlon, p, o, c):
    fields, height, width = p.shape
    chunks = pl.cdiv(fields, PAIRS)
    blocks = width // LANES
    padded = pl.cdiv(fields, 16) * 16
    vmem = pl.BlockSpec(memory_space=pltpu.VMEM)
    bf16, f32 = jnp.bfloat16, jnp.float32
    g, h = pl.pallas_call(
        functools.partial(exchange_kernel, nlat, nlon),
        out_shape=(
            jax.ShapeDtypeStruct((2, chunks, height + 16, LANES), f32),
            jax.ShapeDtypeStruct((2, 2, padded, width), f32),
        ),
        in_specs=[vmem] * 3,
        out_specs=(vmem, vmem),
        scratch_shapes=[
            pltpu.VMEM((2, 3, blocks, fields * 8, LANES), f32),
            pltpu.VMEM((3, chunks, height, LANES), bf16),
            pltpu.VMEM((3, chunks, 8, LANES), bf16),
            pltpu.VMEM((3, chunks, 8, LANES), bf16),
            pltpu.VMEM((2, 3, padded, width), bf16),
            pltpu.VMEM((2, 3, chunks, height, LANES), bf16),
            pltpu.VMEM((4, 3, chunks, 8, LANES), bf16),
            pltpu.VMEM((2, 3, padded, width), bf16),
            pltpu.SemaphoreType.DMA((8,)),
            pltpu.SemaphoreType.DMA((8,)),
        ],
        compiler_params=pltpu.CompilerParams(collective_id=0, has_side_effects=True),
        name="exchange",
    )(p, o, c)

    block = largest_divisor(fields, 80)
    group = largest_divisor(block, 4)
    field_block = pl.BlockSpec((block, height, width), lambda i: (i, 0, 0))
    lanes_out = pl.cdiv(fields, LANES) * LANES
    m, s = pl.pallas_call(
        functools.partial(stencil_kernel, nlat, group),
        grid=(fields // block,),
        out_shape=(
            jax.ShapeDtypeStruct((fields, height, width), bf16),
            jax.ShapeDtypeStruct((8, lanes_out), f32),
        ),
        in_specs=[field_block] * 3 + [vmem] * 2,
        out_specs=(field_block, pl.BlockSpec((8, lanes_out), lambda i: (0, 0))),
        scratch_shapes=[
            pltpu.VMEM((group, 2, height + 16, width), f32),
            pltpu.VMEM((6, fields * 8, LANES), f32),
            pltpu.VMEM((2, height, width), f32),
        ],
        compiler_params=pltpu.CompilerParams(dimension_semantics=("arbitrary",)),
        name="stencil",
    )(p, o, c, g, h)

    e, a = pl.pallas_call(
        functools.partial(total_kernel, nlat, nlon, float(nlat * height * nlon * width)),
        out_shape=(jax.ShapeDtypeStruct((1, fields), f32), jax.ShapeDtypeStruct((1, fields), f32)),
        in_specs=[vmem],
        out_specs=(vmem, vmem),
        scratch_shapes=[
            pltpu.VMEM((nlon, 8, lanes_out), f32),
            pltpu.VMEM((nlat, 8, lanes_out), f32),
            pltpu.VMEM((8, lanes_out), f32),
            pltpu.SemaphoreType.DMA((nlon,)),
            pltpu.SemaphoreType.DMA((nlon,)),
            pltpu.SemaphoreType.DMA((nlat,)),
            pltpu.SemaphoreType.DMA((nlat,)),
        ],
        compiler_params=pltpu.CompilerParams(collective_id=1, has_side_effects=True),
        name="total",
    )(s)
    return m, e.reshape(fields), a.reshape(fields)


def solution(mesh):
    spec = P(None, "lat", "lon")
    return jax.shard_map(
        functools.partial(local, mesh.shape["lat"], mesh.shape["lon"]),
        mesh=mesh,
        in_specs=(spec, spec, spec),
        out_specs=(spec, P(), P()),
        check_vma=False,
    )
```

```python
import functools

import jax
import jax.numpy as jnp
import numpy as np
from jax import lax
from jax.experimental import pallas as pl
from jax.experimental.pallas import tpu as pltpu
from jax.sharding import PartitionSpec as P

MESH = pl.DeviceIdType.MESH
LANES = 128
PAIRS = LANES // 2
epsilon = 1e-06


def lane_index(shape):
    return lax.broadcasted_iota(jnp.int32, shape, len(shape) - 1)


def around(axis, step, size):
    return lax.rem(lax.axis_index(axis) + (step + size), size)


def plan(fields):
    group = max(d for d in range(1, 7) if fields % d == 0)
    groups = fields // group
    count = -(-groups // (PAIRS // group))
    sizes = [group * ((groups + i) // count) for i in range(count)]
    starts = [sum(sizes[:i]) for i in range(count)]
    return group, list(zip(starts, sizes))


def fused_kernel(
    nlat, nlon, p_hbm, o_hbm, c_hbm, m_hbm, out_ref,
    p_ref, o_ref, c_ref, m_ref, tiles, q, ct, cb, rows, qr, cr, rr, gb, hb, hs, acc, wr, sums, b1, t1, b2,
    load, store, send, recv, send1, recv1, send2, recv2,
):
    fields, height, width = p_ref.shape
    group, chunks = plan(fields)
    blocks = width // LANES
    down, up = around("lat", 1, nlat), around("lat", -1, nlat)
    right, left = around("lon", 1, nlon), around("lon", -1, nlon)
    y, x = lax.axis_index("lat"), lax.axis_index("lon")

    loads = []
    for k, (base, size) in enumerate(chunks):
        cut = pl.ds(base, size)
        loads.append(
            [
                pltpu.make_async_copy(src.at[cut], dst.at[cut], load.at[k, a])
                for a, (src, dst) in enumerate(((p_hbm, p_ref), (o_hbm, o_ref), (c_hbm, c_ref)))
            ]
        )
        for copy in loads[-1]:
            copy.start()

    barrier = pltpu.get_barrier_semaphore()
    greeted = [(y, around("lon", d, nlon)) for d in range(1, nlon)]
    greeted += [(around("lat", d, nlat), x) for d in range(1, nlat)]
    greeted += [(down, right), (down, left), (up, right), (up, left)]
    for target in greeted:
        pl.semaphore_signal(barrier, inc=1, device_id=target, device_id_type=MESH)

    def routes(k, size):
        used = pl.ds(0, -(-size // 16) * 16)
        pairs = [
            (rows.at[k, 1, :, used], rr.at[k, 0, :, used], (down, x)),
            (rows.at[k, 0, :, used], rr.at[k, 1, :, used], (up, x)),
            (q.at[k], qr.at[k, 0], (y, right)),
            (q.at[k], qr.at[k, 1], (y, left)),
            (ct.at[k], cr.at[k, 0], (down, right)),
            (ct.at[k], cr.at[k, 1], (down, left)),
            (cb.at[k], cr.at[k, 2], (up, right)),
            (cb.at[k], cr.at[k, 3], (up, left)),
        ]
        return [
            pltpu.make_async_remote_copy(
                src_ref=src,
                dst_ref=dst,
                send_sem=send.at[k, i],
                recv_sem=recv.at[k, i],
                device_id=target,
                device_id_type=MESH,
            )
            for i, (src, dst, target) in enumerate(pairs)
        ]

    lane = lane_index((height, LANES))
    copies = []
    for k, (base, size) in enumerate(chunks):
        for copy in loads[k]:
            copy.wait()

        def pack(j, totals):
            out = list(totals)
            for u in range(2 if size % 2 == 0 else 1):
                s = j * (2 if size % 2 == 0 else 1) + u
                keep = (lane >> 1) == s
                for a, ref in enumerate((p_ref, o_ref, c_ref)):
                    cells = ref[base + s].astype(jnp.float32)
                    at = pl.multiple_of(s * 8, 8)
                    for b in range(blocks):
                        cut = slice(b * LANES, (b + 1) * LANES)
                        tiles[0, a, b, pl.ds(at, 8), :] = cells[:8, cut]
                        tiles[1, a, b, pl.ds(at, 8), :] = cells[height - 8 :, cut]
                    edge = cells
                    if blocks > 1:
                        edge = jnp.where(lane == 0, cells[:, :LANES], cells[:, width - LANES :])
                    out[a] = jnp.where(keep, pltpu.roll(edge, 2 * s + 1, axis=1), out[a])
            return tuple(out)

        zero = jnp.zeros((height, LANES), jnp.float32)
        packed = lax.fori_loop(0, size // 2 if size % 2 == 0 else size, pack, (zero, zero, zero))
        for a in range(3):
            q[k, a] = packed[a].astype(jnp.bfloat16)
            ct[k, a] = packed[a][height - 8 :].astype(jnp.bfloat16)
            cb[k, a] = packed[a][:8].astype(jnp.bfloat16)
        for side, row in ((0, 0), (1, 7)):
            for a in range(3):
                for b in range(blocks):
                    line = tiles[side, a, b, pl.ds(row, PAIRS, stride=8), :]
                    rows[k, side, a, :, b * LANES : (b + 1) * LANES] = line.astype(jnp.bfloat16)
        if k == 0:
            pl.semaphore_wait(barrier, len(greeted))
        copies.append(routes(k, size))
        for copy in copies[k]:
            copy.start()

    total_rows = nlat * height
    row = y * height + lax.broadcasted_iota(jnp.int32, (height, width), 0)
    spots = np.arange(total_rows, dtype=np.float64) / (total_rows - 1)
    mean = float(np.mean(np.cos(np.pi * (0.5 - spots))))
    place = row.astype(jnp.float32) / (total_rows - 1)
    wr[0] = jnp.cos(jnp.pi * (0.5 - place)) / mean
    count = 3.0 - (row == 0).astype(jnp.float32) - (row == total_rows - 1).astype(jnp.float32)
    wr[1] = 1.0 / (3.0 * count)

    inside = ((y > 0).astype(jnp.float32), (y < nlat - 1).astype(jnp.float32))

    def merged(west, east):
        shape = west[0].shape
        even = (lane_index(shape) & 1) == 0
        picked = [jnp.where(even, l.astype(jnp.float32), r.astype(jnp.float32)) for l, r in zip(west, east)]
        out = []
        for a in range(2):
            d = picked[a] - picked[2]
            out.append(jnp.where(even, pltpu.roll(d, LANES - 1, axis=1), pltpu.roll(d, 1, axis=1)))
        return out

    wide = lane_index((PAIRS, width))
    full = lane_index((height, width))
    first, last = full == 0, full == width - 1
    thin = lane_index((1, width))
    ends = (thin == 0) | (thin == width - 1)
    stores = []
    for k, (base, size) in enumerate(chunks):
        for copy in copies[k]:
            copy.wait_recv()
        mid = merged([qr[k, 0, a] for a in range(3)], [qr[k, 1, a] for a in range(3)])
        top = merged([cr[k, 0, a] for a in range(3)], [cr[k, 1, a] for a in range(3)])
        bottom = merged([cr[k, 2, a] for a in range(3)], [cr[k, 3, a] for a in range(3)])
        for a in range(2):
            gb[a, 0:8, :] = top[a] * inside[0]
            gb[a, 8 : 8 + height, :] = mid[a]
            gb[a, 8 + height :, :] = bottom[a] * inside[1]
        for side in range(2):
            line = [rr[k, side, a].astype(jnp.float32) for a in range(3)]
            for a in range(2):
                d = line[a] - line[2]
                before = jnp.where(wide == 0, 0.0, pltpu.roll(d, 1, axis=1))
                after = jnp.where(wide == width - 1, 0.0, pltpu.roll(d, width - 1, axis=1))
                hb[a, side] = (d + before + after) * inside[side]

        def body(g, carry):
            for u in range(group):
                j = g * group + u
                normal = c_ref[base + j].astype(jnp.float32)
                for a, ref in enumerate((p_ref, o_ref)):
                    d = ref[base + j].astype(jnp.float32) - normal
                    edge = pltpu.roll(gb[a], LANES - 1 - 2 * j, axis=1)
                    if blocks > 1:
                        edge = jnp.concatenate([edge] * blocks, axis=1)
                    beside = edge[8 : 8 + height]
                    hs[u, a, 8 : 8 + height, :] = (
                        d
                        + jnp.where(first, beside, pltpu.roll(d, 1, axis=1))
                        + jnp.where(last, beside, pltpu.roll(d, width - 1, axis=1))
                    )
                    hs[u, a, 7:8, :] = hb[a, 0, pl.ds(j, 1), :] + jnp.where(ends, edge[7:8], 0.0)
                    hs[u, a, 8 + height : 9 + height, :] = hb[a, 1, pl.ds(j, 1), :] + jnp.where(
                        ends, edge[8 + height : 9 + height], 0.0
                    )
            for u in range(group):
                f = base + g * group + u
                totals = [None] * 6
                for t in range(0, height, 8):
                    weight, inverse = wr[0, t : t + 8], wr[1, t : t + 8]
                    fcst, true = [
                        (hs[u, a, 7 + t : 15 + t, :] + hs[u, a, 8 + t : 16 + t, :] + hs[u, a, 9 + t : 17 + t, :]) * inverse
                        for a in range(2)
                    ]
                    gap = fcst - true
                    m_ref[f, t : t + 8, :] = gap.astype(jnp.bfloat16)
                    wf, wt = weight * fcst, weight * true
                    for i, term in enumerate((weight * gap * gap, wf, wt, wf * fcst, wt * true, wf * true)):
                        totals[i] = term if totals[i] is None else totals[i] + term
                at = pl.multiple_of(f * 8, 8)
                for i in range(6):
                    part = totals[i]
                    if blocks > 1:
                        part = sum(part[:, b * LANES : (b + 1) * LANES] for b in range(blocks))
                    acc[i, pl.ds(at, 8), :] = part
            return carry

        lax.fori_loop(0, size // group, body, 0)
        cut = pl.ds(base, size)
        stores.append(pltpu.make_async_copy(m_ref.at[cut], m_hbm.at[cut], store.at[k]))
        stores[-1].start()

    ones = jnp.ones((8, 3 * LANES), jnp.bfloat16)
    sums[...] = jnp.zeros_like(sums)
    for i in range(6):
        part = acc[i, pl.ds(0, fields, stride=8), :]
        for s in range(1, 8):
            part = part + acc[i, pl.ds(s, fields, stride=8), :]
        pieces = []
        for _ in range(3):
            pieces.append(part.astype(jnp.bfloat16))
            part = part - pieces[-1].astype(jnp.float32)
        r = lax.dot_general(
            ones, jnp.concatenate(pieces, axis=1), (((1,), (1,)), ((), ())), preferred_element_type=jnp.float32
        )
        sums[i : i + 1, :fields] = r[:1]

    def stage(src, buf, send, recv, axis, size, me):
        def copy(d, slot):
            peer = around(axis, d, size)
            target = (y, peer) if axis == "lon" else (peer, x)
            return pltpu.make_async_remote_copy(
                src_ref=src,
                dst_ref=buf.at[slot],
                send_sem=send.at[d],
                recv_sem=recv.at[slot],
                device_id=target,
                device_id_type=MESH,
            )

        for d in range(1, size):
            copy(d, me).start()
        buf[me] = src[...]
        for d in range(1, size):
            copy(d, around(axis, -d, size)).wait_recv()
        total = buf[0]
        for i in range(1, size):
            total = total + buf[i]
        return total, lambda: [copy(d, me).wait_send() for d in range(1, size)]

    t1[...], sent1 = stage(sums, b1, send1, recv1, "lon", nlon, x)
    out_ref[...], sent2 = stage(t1, b2, send2, recv2, "lat", nlat, y)
    sent1()
    sent2()
    for chunk in copies:
        for copy in chunk:
            copy.wait_send()
    for copy in stores:
        copy.wait()


def finish(totals, cells):
    part = totals / cells
    variance_fcst = part[3] - part[1] * part[1]
    variance_true = part[4] - part[2] * part[2]
    covariance = part[5] - part[1] * part[2]
    return jnp.sqrt(part[0]), covariance / jnp.sqrt((variance_fcst + epsilon) * (variance_true + epsilon))


def local(nlat, nlon, p, o, c):
    fields, height, width = p.shape
    group, chunks = plan(fields)
    n = len(chunks)
    blocks = width // LANES
    lanes_out = pl.cdiv(fields, LANES) * LANES
    bf16, f32 = jnp.bfloat16, jnp.float32
    anywhere = pl.BlockSpec(memory_space=pl.ANY)
    m, s = pl.pallas_call(
        functools.partial(fused_kernel, nlat, nlon),
        out_shape=(
            jax.ShapeDtypeStruct((fields, height, width), bf16),
            jax.ShapeDtypeStruct((8, lanes_out), f32),
        ),
        in_specs=[anywhere] * 3,
        out_specs=(anywhere, pl.BlockSpec(memory_space=pltpu.VMEM)),
        scratch_shapes=[
            *[pltpu.VMEM((fields, height, width), bf16)] * 4,
            pltpu.VMEM((2, 3, blocks, PAIRS * 8, LANES), f32),
            pltpu.VMEM((n, 3, height, LANES), bf16),
            pltpu.VMEM((n, 3, 8, LANES), bf16),
            pltpu.VMEM((n, 3, 8, LANES), bf16),
            pltpu.VMEM((n, 2, 3, PAIRS, width), bf16),
            pltpu.VMEM((n, 2, 3, height, LANES), bf16),
            pltpu.VMEM((n, 4, 3, 8, LANES), bf16),
            pltpu.VMEM((n, 2, 3, PAIRS, width), bf16),
            pltpu.VMEM((2, height + 16, LANES), f32),
            pltpu.VMEM((2, 2, PAIRS, width), f32),
            pltpu.VMEM((group, 2, height + 16, width), f32),
            pltpu.VMEM((6, fields * 8, LANES), f32),
            pltpu.VMEM((2, height, width), f32),
            pltpu.VMEM((8, lanes_out), f32),
            pltpu.VMEM((nlon, 8, lanes_out), f32),
            pltpu.VMEM((8, lanes_out), f32),
            pltpu.VMEM((nlat, 8, lanes_out), f32),
            pltpu.SemaphoreType.DMA((n, 3)),
            pltpu.SemaphoreType.DMA((n,)),
            pltpu.SemaphoreType.DMA((n, 8)),
            pltpu.SemaphoreType.DMA((n, 8)),
            pltpu.SemaphoreType.DMA((nlon,)),
            pltpu.SemaphoreType.DMA((nlon,)),
            pltpu.SemaphoreType.DMA((nlat,)),
            pltpu.SemaphoreType.DMA((nlat,)),
        ],
        compiler_params=pltpu.CompilerParams(collective_id=0, has_side_effects=True),
        name="fused",
    )(p, o, c)
    e, a = finish(s[:, :fields], float(nlat * height * nlon * width))
    return m, e, a


def solution(mesh):
    spec = P(None, "lat", "lon")
    return jax.shard_map(
        functools.partial(local, mesh.shape["lat"], mesh.shape["lon"]),
        mesh=mesh,
        in_specs=(spec, spec, spec),
        out_specs=(spec, P(), P()),
        check_vma=False,
    )
```
